32 devices in a mesh: bank: 4 (over z), zero: 8 (over y, x, core).
Axes of the slice: x: 2, y: 2, z: 4, core: 2. Of those that a mesh axis runs over, the one named last changes fastest.
Arguments:
- w_gate: float32 [128, 2048, 768], P('bank', 'zero'), may hold values from -0.1875 to 0.1875
- w_up: float32 [128, 2048, 768], P('bank', 'zero'), may hold values from -0.1875 to 0.1875
- router_weight: float32 [2048, 128], P('zero', 'bank'), may hold values from -0.125 to 0.125
- router_gain: float32 [2048], P('zero'), may hold values from 0.25 to 1.75
Outputs:
- serve_gate: bfloat16 [128, 2048, 768], P('bank', None, 'zero')
- serve_up: bfloat16 [128, 2048, 768], P('bank', None, 'zero')
- scale_gate: float32 [128, 768], P('bank', 'zero')
- scale_up: float32 [128, 768], P('bank', 'zero')
- serve_router: bfloat16 [2048, 128], replicated
The draws below stay inside these ranges and needn't reach their ends.
All inputs are finite; a program needn't handle non-finite values.
Results may differ from the reference program's by a relative error of at most 0.001.
Values may be sent and summed in bfloat16 or wider, within the bound.
No kernel may reach another device: no remote copies, remote signals or barrier semaphores. Data moves between devices by JAX's collectives and lax.ppermute only.
A program may use at most 192 MiB of HBM per device.

```python
import jax
import jax.numpy as jnp
from jax import lax

EXPERTS = 128
D_MODEL = 2048
D_EXPERT = 768


def strengthened(drawn, own_key, source, target, shards_of, factor):
    owner, partner = [(jnp.arange(drawn.shape[position]) // (drawn.shape[position] // shards_of)).reshape([-1 if axis == position else 1 for axis in range(drawn.ndim)]) for position in (source, target)]
    chosen = jax.random.permutation(own_key, shards_of)[partner]
    strong = (owner == chosen) | (owner == (partner + shards_of // 2) % shards_of)
    return jnp.where(strong, factor * drawn, drawn)


def block_levels(key, shape, shards, least, top_value):
    gain, own = 1.0, jax.random.fold_in(key, 6)
    for dim, blocks in shards:
        steps = jnp.exp(jax.random.uniform(jax.random.fold_in(own, dim), (blocks,), jnp.float32, least / len(shards), top_value / len(shards)))
        gain = gain * jnp.repeat(steps, shape[dim] // blocks).reshape([-1 if axis == dim else 1 for axis in range(len(shape))])
    return gain


def noise(stream_key, shape, spread, limit, cuts=(), dtype=jnp.bfloat16):
    result = jax.random.normal(stream_key, shape, jnp.float32) * spread
    if len(cuts) > 0:
        result = block_levels(stream_key, shape, cuts, -0.22, 0.18) * result
    return jnp.clip(result, min=-limit, max=limit).astype(dtype)


def bell_draw_with(key, extent, scale, limit, shards, heavy, held_as=jnp.bfloat16):
    drawn = scale * jax.random.normal(key, extent, jnp.float32)
    if shards:
        drawn = drawn * block_levels(key, extent, shards, -0.22, 0.18)
    return jnp.clip(strengthened(drawn, jax.random.fold_in(key, 3), *heavy), -limit, limit).astype(held_as)


def setup_inputs(seed: int = 0) -> dict:
    streams_of = jax.random.split(jax.random.key(seed), 5)
    return {
        "w_gate": bell_draw_with(streams_of[0], (EXPERTS, D_MODEL, D_EXPERT), D_MODEL ** -0.5, 0.1875, ((0, 4), (1, 8)), (1, 2, 8, 2.0), jnp.float32),
        "w_up": bell_draw_with(streams_of[1], (EXPERTS, D_MODEL, D_EXPERT), D_MODEL ** -0.5, 0.1875, ((0, 4), (1, 8)), (1, 2, 8, 2.0), jnp.float32),
        "router_weight": noise(streams_of[2], (D_MODEL, EXPERTS), D_MODEL ** -0.5, 0.125, ((0, 8), (1, 4)), jnp.float32),
        "router_gain": jnp.clip(1.0 + 0.15 * jax.random.normal(streams_of[3], (D_MODEL,), jnp.float32), 0.25, 1.75),
    }


def reference(w_gate, w_up, router_weight, router_gain):
    scale_gate = jnp.sqrt(lax.optimization_barrier(jnp.sum(w_gate * w_gate, axis=1)))
    serve_gate = (w_gate / jnp.expand_dims(scale_gate, 1)).astype(jnp.bfloat16)
    scale_up = jnp.sqrt(lax.optimization_barrier(jnp.sum(w_up * w_up, axis=1)))
    serve_up = (w_up / jnp.expand_dims(scale_up, 1)).astype(jnp.bfloat16)
    serve_router = (router_weight * router_gain[:, None]).astype(jnp.bfloat16)
    return (serve_gate, serve_up, scale_gate, scale_up, serve_router)
```

```python
import jax
import jax.numpy as jnp
from jax import lax
from jax.experimental import pallas as pl
from jax.experimental.pallas import tpu as pltpu
from jax.sharding import PartitionSpec as P


def xor_pairs(size, k):
    return [(i, i ^ k) for i in range(size)]


def cost(flops, moved):
    return pl.CostEstimate(flops=flops, bytes_accessed=moved, transcendentals=0)


def square_sums(w_gate, w_up, first, count):
    _, rows, cols = w_gate.shape
    per_step = 2 if count % 2 == 0 and first % 2 == 0 else 1

    def kernel(gate_ref, up_ref, out_ref):
        step = pl.program_id(0)
        for n in range(per_step):
            for side, ref in enumerate((gate_ref, up_ref)):
                w = ref[n]
                out_ref[side, pl.ds(step * per_step + n, 1), :] = jnp.sum(w * w, axis=0, keepdims=True)

    weights = pl.BlockSpec((per_step, rows, cols), lambda i: (first // per_step + i, 0, 0))
    return pl.pallas_call(
        kernel,
        grid=(count // per_step,),
        in_specs=[weights, weights],
        out_specs=pl.BlockSpec((2, count, cols), lambda i: (0, 0, 0)),
        out_shape=jax.ShapeDtypeStruct((2, count, cols), jnp.float32),
        cost_estimate=cost(4 * count * rows * cols, 8 * count * rows * cols),
    )(w_gate, w_up)


def scaled_pieces(w_gate, w_up, total, first, count, start, size):
    _, rows, cols = w_gate.shape
    width = cols // size

    def kernel(gate_ref, up_ref, total_ref, *refs):
        outs, held = refs[:size], refs[size]
        me = lax.axis_index("zero")
        step = pl.program_id(0)
        for side, ref in enumerate((gate_ref, up_ref)):
            inverse = 1.0 / jnp.sqrt(total_ref[side, pl.ds(start + step, 1), :])
            held[side] = (ref[0] * inverse).astype(jnp.bfloat16).T
            for k in range(size):
                offset = pl.multiple_of(lax.bitwise_xor(me, k) * width, width)
                outs[k][side, 0] = held[side, pl.ds(offset, width), :]

    weights = pl.BlockSpec((1, rows, cols), lambda i: (first + i, 0, 0))
    piece = pl.BlockSpec((2, 1, width, rows), lambda i: (0, i, 0, 0))
    return pl.pallas_call(
        kernel,
        grid=(count,),
        in_specs=[weights, weights, pl.BlockSpec(total.shape, lambda i: (0, 0, 0))],
        out_specs=[piece] * size,
        out_shape=[jax.ShapeDtypeStruct((2, count, width, rows), jnp.bfloat16)] * size,
        scratch_shapes=[pltpu.VMEM((2, cols, rows), jnp.bfloat16)],
        cost_estimate=cost(4 * count * rows * cols, 12 * count * rows * cols),
    )(w_gate, w_up, total)


def assembled(pieces, outputs, first, experts):
    size = len(pieces)
    _, count, width, rows = pieces[0].shape

    def kernel(*refs):
        ins, outs = refs[:size], refs[-2:]
        me = lax.axis_index("zero")
        for k in range(size):
            offset = pl.multiple_of(lax.bitwise_xor(me, k) * rows, rows)
            for side in range(2):
                outs[side][0, :, pl.ds(offset, rows)] = ins[k][side, 0]

    piece = pl.BlockSpec((2, 1, width, rows), lambda i: (0, i, 0, 0))
    whole = pl.BlockSpec((1, width, size * rows), lambda i: (first + i, 0, 0))
    kept = () if outputs is None else tuple(outputs)
    return pl.pallas_call(
        kernel,
        grid=(count,),
        in_specs=[piece] * size + [pl.BlockSpec(memory_space=pl.ANY)] * len(kept),
        out_specs=[whole, whole],
        out_shape=[jax.ShapeDtypeStruct((experts, width, size * rows), jnp.bfloat16)] * 2,
        input_output_aliases={size + n: n for n in range(len(kept))},
        cost_estimate=cost(count * width * rows * size, 8 * count * width * rows * size),
    )(*pieces, *kept)


def joined_rows(pieces):
    size = len(pieces)
    height, rows = pieces[0].shape

    def kernel(*refs):
        me = lax.axis_index("zero")
        for k in range(size):
            offset = pl.multiple_of(lax.bitwise_xor(me, k) * rows, rows)
            refs[size][:, pl.ds(offset, rows)] = refs[k][...]

    return pl.pallas_call(
        kernel,
        out_shape=jax.ShapeDtypeStruct((height, size * rows), pieces[0].dtype),
        cost_estimate=cost(size * height * rows, 4 * size * height * rows),
    )(*pieces)


def joined_columns(pieces):
    banks = len(pieces)
    height, rows = pieces[0].shape

    def kernel(*refs):
        out_ref, held = refs[banks], refs[banks + 1]
        me = lax.axis_index("bank")
        for k in range(banks):
            offset = pl.multiple_of(lax.bitwise_xor(me, k) * height, height)
            held[pl.ds(offset, height), :] = refs[k][...]
        out_ref[...] = held[...].T

    return pl.pallas_call(
        kernel,
        out_shape=jax.ShapeDtypeStruct((rows, banks * height), pieces[0].dtype),
        scratch_shapes=[pltpu.VMEM((banks * height, rows), pieces[0].dtype)],
        cost_estimate=cost(banks * height * rows, 4 * banks * height * rows),
    )(*pieces)


def chunk_sizes(experts):
    sizes, left = [], experts
    for part in (16, 8, 4, 4, 4, 8, 16):
        take = max(1, experts // part)
        sizes.append(min(take, left))
        left -= sizes[-1]
    if left:
        sizes[len(sizes) // 2] += left
    return [n for n in sizes if n]


def piped(w_gate, w_up, router_weight, router_gain, size, banks):
    experts, _, cols = w_gate.shape
    width = cols // size

    def send(x, k, axis="zero", count=size):
        return lax.ppermute(x, axis, xor_pairs(count, k))

    total = square_sums(w_gate, w_up, 0, experts)
    k = 1
    while k < size:
        total = total + send(total, k)
        k *= 2

    sizes = chunk_sizes(experts)
    chunks = range(len(sizes))
    firsts = [sum(sizes[:c]) for c in chunks]
    sent, got = [], [dict() for _ in chunks]
    for c in chunks:
        sent.append(scaled_pieces(w_gate, w_up, total, firsts[c], sizes[c], firsts[c], size))
        got[c] = [sent[c][0]] + [send(sent[c][k], k) for k in range(1, size)]

    part = (router_weight * router_gain[:, None]).astype(jnp.bfloat16).T
    row = joined_rows([part] + [send(part, k) for k in range(1, size)])
    columns = [row] + [send(row, k, "bank", banks) for k in range(1, banks)]
    serve_router = joined_columns(columns)

    outputs = None
    for c in chunks:
        outputs = assembled(got[c], outputs, firsts[c], experts)
    serve_gate, serve_up = (jnp.swapaxes(x, 1, 2) for x in outputs)

    mine = lax.dynamic_slice_in_dim(total, lax.axis_index("zero") * width, width, axis=2)
    scale = jnp.sqrt(mine)
    return (serve_gate, serve_up, scale[0], scale[1], serve_router)


def plain(w_gate, w_up, router_weight, router_gain):
    total_gate, total_up = lax.psum(
        (jnp.sum(w_gate * w_gate, axis=1), jnp.sum(w_up * w_up, axis=1)), "zero"
    )
    scale_gate, scale_up = jnp.sqrt(total_gate), jnp.sqrt(total_up)
    served = [
        lax.all_to_all(
            (w / jnp.expand_dims(scale, 1)).astype(jnp.bfloat16), "zero", split_axis=2, concat_axis=1, tiled=True
        )
        for w, scale in ((w_gate, scale_gate), (w_up, scale_up))
    ]
    width = served[0].shape[2]
    start = lax.axis_index("zero") * width
    scales = [lax.dynamic_slice_in_dim(s, start, width, axis=1) for s in (scale_gate, scale_up)]
    part = (router_weight * router_gain[:, None]).astype(jnp.bfloat16)
    row = lax.all_gather(part, "zero", axis=0, tiled=True)
    return (*served, *scales, lax.all_gather(row, "bank", axis=1, tiled=True))


def solution(mesh):
    size, banks = mesh.shape["zero"], mesh.shape["bank"]
    placed = (P("bank", "zero", None), P("bank", "zero", None), P("zero", "bank"), P("zero"))

    def placed_over(shards):
        return jax.shard_map(
            shards,
            mesh=mesh,
            in_specs=placed,
            out_specs=(
                P("bank", None, "zero"),
                P("bank", None, "zero"),
                P("bank", "zero"),
                P("bank", "zero"),
                P(),
            ),
            check_vma=False,
        )

    def whole(w_gate, w_up, router_weight, router_gain):
        _, rows, cols = w_gate.shape
        powers = size & (size - 1) == 0 and banks & (banks - 1) == 0
        aligned = rows % (128 * size) == 0 and cols % (16 * size) == 0 and router_weight.shape[1] % (16 * banks) == 0
        if not (powers and aligned and size >= 8):
            return placed_over(plain)(w_gate, w_up, router_weight, router_gain)

        def shards(*args):
            return piped(*args, size, banks)

        return placed_over(shards)(w_gate, w_up, router_weight, router_gain)

    return whole
```

```python
import jax
import jax.numpy as jnp
from jax import lax
from jax.experimental import pallas as pl
from jax.experimental.pallas import tpu as pltpu
from jax.sharding import PartitionSpec as P


def xor_pairs(size, k):
    return [(i, i ^ k) for i in range(size)]


def granted(mib):
    return pltpu.CompilerParams(vmem_limit_bytes=mib << 20)


def cost(flops, moved):
    return pl.CostEstimate(flops=flops, bytes_accessed=moved, transcendentals=0)


def square_sums(w_gate, w_up, first, count):
    _, rows, cols = w_gate.shape
    per_step = 2

    def kernel(gate_ref, up_ref, out_ref):
        step = pl.program_id(0)
        for n in range(per_step):
            for side, ref in enumerate((gate_ref, up_ref)):
                w = ref[n]
                out_ref[side, pl.ds(step * per_step + n, 1), :] = jnp.sum(w * w, axis=0, keepdims=True)

    weights = pl.BlockSpec((per_step, rows, cols), lambda i: (first // per_step + i, 0, 0))
    return pl.pallas_call(
        kernel,
        grid=(count // per_step,),
        in_specs=[weights, weights],
        out_specs=pl.BlockSpec((2, count, cols), lambda i: (0, 0, 0)),
        out_shape=jax.ShapeDtypeStruct((2, count, cols), jnp.float32),
        compiler_params=granted(44),
        cost_estimate=cost(4 * count * rows * cols, 8 * count * rows * cols),
    )(w_gate, w_up)


def scaled_pieces(w_gate, w_up, totals, first, count, start, size):
    _, rows, cols = w_gate.shape
    width = cols // size

    def kernel(gate_ref, up_ref, *refs):
        total_refs, outs, held = refs[: len(totals)], refs[len(totals) : -1], refs[-1]
        me = lax.axis_index("zero")
        step = pl.program_id(0)
        for side, w_ref in enumerate((gate_ref, up_ref)):
            total = sum(ref[side, pl.ds(start + step, 1), :] for ref in total_refs)
            inverse = 1.0 / jnp.sqrt(total)
            held[side] = (w_ref[0] * inverse).astype(jnp.bfloat16).T
            for k in range(size):
                offset = pl.multiple_of(lax.bitwise_xor(me, k) * width, width)
                outs[k][side, 0] = held[side, pl.ds(offset, width), :]

    weights = pl.BlockSpec((1, rows, cols), lambda i: (first + i, 0, 0))
    piece = pl.BlockSpec((2, 1, width, rows), lambda i: (0, i, 0, 0))
    return pl.pallas_call(
        kernel,
        grid=(count,),
        in_specs=[weights, weights] + [pl.BlockSpec(memory_space=pltpu.VMEM)] * len(totals),
        out_specs=[piece] * size,
        out_shape=[jax.ShapeDtypeStruct((2, count, width, rows), jnp.bfloat16)] * size,
        scratch_shapes=[pltpu.VMEM((2, cols, rows), jnp.bfloat16)],
        compiler_params=granted(44),
        cost_estimate=cost(4 * count * rows * cols, 12 * count * rows * cols),
    )(w_gate, w_up, *totals)


def assembled(pieces, outputs, first, experts):
    size = len(pieces)
    _, count, width, rows = pieces[0].shape

    def kernel(*refs):
        ins, outs = refs[:size], refs[-2:]
        me = lax.axis_index("zero")
        for k in range(size):
            offset = pl.multiple_of(lax.bitwise_xor(me, k) * rows, rows)
            for side in range(2):
                outs[side][0, :, pl.ds(offset, rows)] = ins[k][side, 0]

    piece = pl.BlockSpec((2, 1, width, rows), lambda i: (0, i, 0, 0))
    whole = pl.BlockSpec((1, width, size * rows), lambda i: (first + i, 0, 0))
    kept = () if outputs is None else tuple(outputs)
    return pl.pallas_call(
        kernel,
        grid=(count,),
        in_specs=[piece] * size + [pl.BlockSpec(memory_space=pl.ANY)] * len(kept),
        out_specs=[whole, whole],
        out_shape=[jax.ShapeDtypeStruct((experts, width, size * rows), jnp.bfloat16)] * 2,
        input_output_aliases={size + n: n for n in range(len(kept))},
        compiler_params=granted(44),
        cost_estimate=cost(count * width * rows * size, 8 * count * width * rows * size),
    )(*pieces, *kept)


def joined_rows(pieces):
    size = len(pieces)
    height, rows = pieces[0].shape

    def kernel(*refs):
        me = lax.axis_index("zero")
        for k in range(size):
            offset = pl.multiple_of(lax.bitwise_xor(me, k) * rows, rows)
            refs[size][:, pl.ds(offset, rows)] = refs[k][...]

    return pl.pallas_call(
        kernel,
        out_shape=jax.ShapeDtypeStruct((height, size * rows), pieces[0].dtype),
        cost_estimate=cost(size * height * rows, 4 * size * height * rows),
    )(*pieces)


def joined_columns(pieces):
    banks = len(pieces)
    height, rows = pieces[0].shape

    def kernel(*refs):
        out_ref, held = refs[banks], refs[banks + 1]
        me = lax.axis_index("bank")
        for k in range(banks):
            offset = pl.multiple_of(lax.bitwise_xor(me, k) * height, height)
            held[pl.ds(offset, height), :] = refs[k][...]
        out_ref[...] = held[...].T

    return pl.pallas_call(
        kernel,
        out_shape=jax.ShapeDtypeStruct((rows, banks * height), pieces[0].dtype),
        scratch_shapes=[pltpu.VMEM((banks * height, rows), pieces[0].dtype)],
        cost_estimate=cost(banks * height * rows, 4 * banks * height * rows),
    )(*pieces)


def chunk_sizes(experts):
    unit = experts // 32
    return [[unit * n for n in group] for group in ((2,), (2, 4), (4, 8, 8, 3, 1))]


def piped(w_gate, w_up, router_weight, router_gain, size, banks):
    experts, _, cols = w_gate.shape
    width = cols // size

    def send(x, k, axis="zero", count=size):
        return lax.ppermute(x, axis, xor_pairs(count, k))

    groups = chunk_sizes(experts)
    sizes = [n for group in groups for n in group]
    chunks = range(len(sizes))
    firsts = [sum(sizes[:c]) for c in chunks]

    totals, starts = [], [sum(map(sum, groups[:g])) for g in range(len(groups))]
    for g, group in enumerate(groups):
        own = square_sums(w_gate, w_up, starts[g], sum(group))
        own = own + send(own, 1)
        totals.append([own] + [send(own, k) for k in range(2, size, 2)])

    sent, got = [], []
    for c in chunks:
        group = max(g for g in range(len(groups)) if starts[g] <= firsts[c])
        start = firsts[c] - starts[group]
        sent.append(scaled_pieces(w_gate, w_up, totals[group], firsts[c], sizes[c], start, size))
        got.append([sent[c][0]] + [send(sent[c][k], k) for k in range(1, size)])

    part = (router_weight * router_gain[:, None]).astype(jnp.bfloat16).T
    parts = [part] + [send(part, k) for k in range(1, size)]
    row = joined_rows(parts)
    columns = [row] + [send(row, k, "bank", banks) for k in range(1, banks)]
    serve_router = joined_columns(columns)

    outputs = None
    for c in chunks:
        outputs = assembled(got[c], outputs, firsts[c], experts)
    serve_gate, serve_up = (jnp.swapaxes(x, 1, 2) for x in outputs)

    mine = [
        lax.dynamic_slice_in_dim(sum(parts), lax.axis_index("zero") * width, width, axis=2) for parts in totals
    ]
    scale = jnp.sqrt(jnp.concatenate(mine, axis=1))
    return (serve_gate, serve_up, scale[0], scale[1], serve_router)


def plain(w_gate, w_up, router_weight, router_gain):
    total_gate, total_up = lax.psum(
        (jnp.sum(w_gate * w_gate, axis=1), jnp.sum(w_up * w_up, axis=1)), "zero"
    )
    scale_gate, scale_up = jnp.sqrt(total_gate), jnp.sqrt(total_up)
    served = [
        lax.all_to_all(
            (w / jnp.expand_dims(scale, 1)).astype(jnp.bfloat16), "zero", split_axis=2, concat_axis=1, tiled=True
        )
        for w, scale in ((w_gate, scale_gate), (w_up, scale_up))
    ]
    width = served[0].shape[2]
    start = lax.axis_index("zero") * width
    scales = [lax.dynamic_slice_in_dim(s, start, width, axis=1) for s in (scale_gate, scale_up)]
    part = (router_weight * router_gain[:, None]).astype(jnp.bfloat16)
    row = lax.all_gather(part, "zero", axis=0, tiled=True)
    return (*served, *scales, lax.all_gather(row, "bank", axis=1, tiled=True))


def solution(mesh):
    size, banks = mesh.shape["zero"], mesh.shape["bank"]
    placed = (P("bank", "zero", None), P("bank", "zero", None), P("zero", "bank"), P("zero"))

    def placed_over(shards):
        return jax.shard_map(
            shards,
            mesh=mesh,
            in_specs=placed,
            out_specs=(
                P("bank", None, "zero"),
                P("bank", None, "zero"),
                P("bank", "zero"),
                P("bank", "zero"),
                P(),
            ),
            check_vma=False,
        )

    def whole(w_gate, w_up, router_weight, router_gain):
        experts, rows, cols = w_gate.shape
        powers = size & (size - 1) == 0 and banks & (banks - 1) == 0
        aligned = rows % (128 * size) == 0 and cols % (16 * size) == 0 and router_weight.shape[1] % (16 * banks) == 0
        if not (powers and aligned and size >= 8 and experts % (32 * banks) == 0):
            return placed_over(plain)(w_gate, w_up, router_weight, router_gain)

        def shards(*args):
            return piped(*args, size, banks)

        return placed_over(shards)(w_gate, w_up, router_weight, router_gain)

    return whole
```

```python
import jax
import jax.numpy as jnp
from jax import lax
from jax.experimental import pallas as pl
from jax.experimental.pallas import tpu as pltpu
from jax.sharding import PartitionSpec as P


def xor_pairs(size, k):
    return [(i, i ^ k) for i in range(size)]


def granted(mib):
    return pltpu.CompilerParams(vmem_limit_bytes=mib << 20)


def cost(flops, moved):
    return pl.CostEstimate(flops=flops, bytes_accessed=moved, transcendentals=0)


def fetches(sources, first, held, arrived, n):
    return [
        pltpu.make_async_copy(source.at[first + n], held.at[n, side], arrived.at[n, side])
        for side, source in enumerate(sources)
    ]


def square_sums(w_gate, w_up, first, count, halved=False):
    _, rows, cols = w_gate.shape
    results = 2 if halved else 1
    height = count // results

    def kernel(*refs):
        sources, out_refs, (held, arrived) = refs[:2], refs[2:-2], refs[-2:]
        for n in range(count):
            for copy in fetches(sources, first, held, arrived, n):
                copy.start()
        mine = lax.axis_index("zero") % 2
        for half in range(results):

            @pl.loop(0, height)
            def _(n):
                row = half * height + n
                for side, copy in enumerate(fetches(sources, first, held, arrived, row)):
                    copy.wait()
                    w = held[row, side]
                    found = jnp.sum(w * w, axis=0, keepdims=True)
                    if halved:

                        @pl.when(mine == half)
                        def _():
                            out_refs[0][side, pl.ds(n, 1), :] = found

                        @pl.when(mine != half)
                        def _():
                            out_refs[1][side, pl.ds(n, 1), :] = found

                    else:
                        out_refs[0][side, pl.ds(n, 1), :] = found

    return pl.pallas_call(
        kernel,
        in_specs=[pl.BlockSpec(memory_space=pl.ANY)] * 2,
        out_specs=[pl.BlockSpec(memory_space=pltpu.VMEM)] * results,
        out_shape=[jax.ShapeDtypeStruct((2, height, cols), jnp.float32)] * results,
        scratch_shapes=[pltpu.VMEM((count, 2, rows, cols), jnp.float32), pltpu.SemaphoreType.DMA((count, 2))],
        compiler_params=granted(44),
        cost_estimate=cost(4 * count * rows * cols, 8 * count * rows * cols),
    )(w_gate, w_up)


def scaled_pieces(w_gate, w_up, totals, halved, first, count, start, size):
    _, rows, cols = w_gate.shape
    width = cols // size

    def kernel(gate_ref, up_ref, *refs):
        total_refs, outs, held = refs[: len(totals)], refs[len(totals) : -1], refs[-1]
        me = lax.axis_index("zero")
        step = pl.program_id(0)
        for side, w_ref in enumerate((gate_ref, up_ref)):
            if halved:
                height = totals[0].shape[1]
                half = jnp.where(start + step >= height, 1, 0)
                row = pl.ds(start + step - half * height, 1)
                total = jnp.where(
                    half == me % 2, total_refs[0][side, row, :], total_refs[1][side, row, :]
                )
            else:
                total = sum(ref[side, pl.ds(start + step, 1), :] for ref in total_refs)
            inverse = 1.0 / jnp.sqrt(total)
            held[side] = (w_ref[0] * inverse).astype(jnp.bfloat16).T
            for k in range(size):
                offset = pl.multiple_of(lax.bitwise_xor(me, k) * width, width)
                outs[k][side, 0] = held[side, pl.ds(offset, width), :]

    weights = pl.BlockSpec((1, rows, cols), lambda i: (first + i, 0, 0))
    piece = pl.BlockSpec((2, 1, width, rows), lambda i: (0, i, 0, 0))
    return pl.pallas_call(
        kernel,
        grid=(count,),
        in_specs=[weights, weights] + [pl.BlockSpec(memory_space=pltpu.VMEM)] * len(totals),
        out_specs=[piece] * size,
        out_shape=[jax.ShapeDtypeStruct((2, count, width, rows), jnp.bfloat16)] * size,
        scratch_shapes=[pltpu.VMEM((2, cols, rows), jnp.bfloat16)],
        compiler_params=granted(44),
        cost_estimate=cost(4 * count * rows * cols, 12 * count * rows * cols),
    )(w_gate, w_up, *totals)


def assembled(pieces, outputs, first, experts):
    size = len(pieces)
    _, count, width, rows = pieces[0].shape

    def kernel(*refs):
        ins, outs = refs[:size], refs[-2:]
        me = lax.axis_index("zero")
        for k in range(size):
            offset = pl.multiple_of(lax.bitwise_xor(me, k) * rows, rows)
            for side in range(2):
                outs[side][0, :, pl.ds(offset, rows)] = ins[k][side, 0]

    piece = pl.BlockSpec((2, 1, width, rows), lambda i: (0, i, 0, 0))
    whole = pl.BlockSpec((1, width, size * rows), lambda i: (first + i, 0, 0))
    kept = () if outputs is None else tuple(outputs)
    return pl.pallas_call(
        kernel,
        grid=(count,),
        in_specs=[piece] * size + [pl.BlockSpec(memory_space=pl.ANY)] * len(kept),
        out_specs=[whole, whole],
        out_shape=[jax.ShapeDtypeStruct((experts, width, size * rows), jnp.bfloat16)] * 2,
        input_output_aliases={size + n: n for n in range(len(kept))},
        compiler_params=granted(44),
        cost_estimate=cost(count * width * rows * size, 8 * count * width * rows * size),
    )(*pieces, *kept)


def joined_rows(pieces):
    size = len(pieces)
    height, rows = pieces[0].shape

    def kernel(*refs):
        me = lax.axis_index("zero")
        for k in range(size):
            offset = pl.multiple_of(lax.bitwise_xor(me, k) * rows, rows)
            refs[size][:, pl.ds(offset, rows)] = refs[k][...]

    return pl.pallas_call(
        kernel,
        out_shape=jax.ShapeDtypeStruct((height, size * rows), pieces[0].dtype),
        cost_estimate=cost(size * height * rows, 4 * size * height * rows),
    )(*pieces)


def joined_columns(pieces):
    banks = len(pieces)
    height, rows = pieces[0].shape

    def kernel(*refs):
        out_ref, held = refs[banks], refs[banks + 1]
        me = lax.axis_index("bank")
        for k in range(banks):
            offset = pl.multiple_of(lax.bitwise_xor(me, k) * height, height)
            held[pl.ds(offset, height), :] = refs[k][...]
        out_ref[...] = held[...].T

    return pl.pallas_call(
        kernel,
        out_shape=jax.ShapeDtypeStruct((rows, banks * height), pieces[0].dtype),
        scratch_shapes=[pltpu.VMEM((banks * height, rows), pieces[0].dtype)],
        cost_estimate=cost(banks * height * rows, 4 * banks * height * rows),
    )(*pieces)


def chunk_sizes(experts):
    unit = experts // 32
    return [[unit * n for n in group] for group in ((2,), (2, 4), (4, 8, 8, 3, 1))]


def piped(w_gate, w_up, router_weight, router_gain, size, banks):
    experts, _, cols = w_gate.shape
    width = cols // size

    def send(x, k, axis="zero", count=size):
        return lax.ppermute(x, axis, xor_pairs(count, k))

    groups = chunk_sizes(experts)
    sizes = [n for group in groups for n in group]
    chunks = range(len(sizes))
    firsts = [sum(sizes[:c]) for c in chunks]

    totals, starts = [], [sum(map(sum, groups[:g])) for g in range(len(groups))]
    last = len(groups) - 1
    for g, group in enumerate(groups[:last]):
        (own,) = square_sums(w_gate, w_up, starts[g], sum(group))
        own = own + send(own, 1)
        totals.append([own] + [send(own, k) for k in range(2, size, 2)])
    own, other = square_sums(w_gate, w_up, starts[last], sum(groups[last]), halved=True)
    own = own + send(other, 1)
    k = 2
    while k < size:
        own = own + send(own, k)
        k *= 2
    totals.append([own, send(own, 1)])

    sent, got = [], []
    for c in chunks:
        group = max(g for g in range(len(groups)) if starts[g] <= firsts[c])
        start = firsts[c] - starts[group]
        sent.append(scaled_pieces(w_gate, w_up, totals[group], group == last, firsts[c], sizes[c], start, size))
        got.append([sent[c][0]] + [send(sent[c][k], k) for k in range(1, size)])

    part = (router_weight * router_gain[:, None]).astype(jnp.bfloat16).T
    parts = [part, send(part, 1)]
    for k in range(2, size, 2):
        parts.append(send(part, k))
        parts.append(send(parts[k], 1))
    row = joined_rows(parts)
    columns = [row] + [send(row, k, "bank", banks) for k in range(1, banks)]
    serve_router = joined_columns(columns)

    outputs = None
    for c in chunks:
        outputs = assembled(got[c], outputs, firsts[c], experts)
    serve_gate, serve_up = (jnp.swapaxes(x, 1, 2) for x in outputs)

    even = lax.axis_index("zero") % 2 == 0
    low, high = (jnp.where(even, x, y) for x, y in (totals[last], totals[last][::-1]))
    mine = [
        lax.dynamic_slice_in_dim(x, lax.axis_index("zero") * width, width, axis=2)
        for x in [sum(parts) for parts in totals[:last]] + [low, high]
    ]
    scale = jnp.sqrt(jnp.concatenate(mine, axis=1))
    return (serve_gate, serve_up, scale[0], scale[1], serve_router)


def plain(w_gate, w_up, router_weight, router_gain):
    total_gate, total_up = lax.psum(
        (jnp.sum(w_gate * w_gate, axis=1), jnp.sum(w_up * w_up, axis=1)), "zero"
    )
    scale_gate, scale_up = jnp.sqrt(total_gate), jnp.sqrt(total_up)
    served = [
        lax.all_to_all(
            (w / jnp.expand_dims(scale, 1)).astype(jnp.bfloat16), "zero", split_axis=2, concat_axis=1, tiled=True
        )
        for w, scale in ((w_gate, scale_gate), (w_up, scale_up))
    ]
    width = served[0].shape[2]
    start = lax.axis_index("zero") * width
    scales = [lax.dynamic_slice_in_dim(s, start, width, axis=1) for s in (scale_gate, scale_up)]
    part = (router_weight * router_gain[:, None]).astype(jnp.bfloat16)
    row = lax.all_gather(part, "zero", axis=0, tiled=True)
    return (*served, *scales, lax.all_gather(row, "bank", axis=1, tiled=True))


def solution(mesh):
    size, banks = mesh.shape["zero"], mesh.shape["bank"]
    placed = (P("bank", "zero", None), P("bank", "zero", None), P("zero", "bank"), P("zero"))

    def placed_over(shards):
        return jax.shard_map(
            shards,
            mesh=mesh,
            in_specs=placed,
            out_specs=(
                P("bank", None, "zero"),
                P("bank", None, "zero"),
                P("bank", "zero"),
                P("bank", "zero"),
                P(),
            ),
            check_vma=False,
        )

    def whole(w_gate, w_up, router_weight, router_gain):
        experts, rows, cols = w_gate.shape
        powers = size & (size - 1) == 0 and banks & (banks - 1) == 0
        aligned = rows % (128 * size) == 0 and cols % (16 * size) == 0 and router_weight.shape[1] % (16 * banks) == 0
        if not (powers and aligned and size >= 8 and experts % (32 * banks) == 0):
            return placed_over(plain)(w_gate, w_up, router_weight, router_gain)

        def shards(*args):
            return piped(*args, size, banks)

        return placed_over(shards)(w_gate, w_up, router_weight, router_gain)

    return whole
```

```python
import jax
import jax.numpy as jnp
from jax import lax
from jax.experimental import pallas as pl
from jax.experimental.pallas import tpu as pltpu
from jax.sharding import PartitionSpec as P


def xor_pairs(size, k):
    return [(i, i ^ k) for i in range(size)]


def granted(mib):
    return pltpu.CompilerParams(vmem_limit_bytes=mib << 20)


def cost(flops, moved):
    return pl.CostEstimate(flops=flops, bytes_accessed=moved, transcendentals=0)


def fetches(sources, first, held, arrived, n):
    return [
        pltpu.make_async_copy(source.at[first + n], held.at[n, side], arrived.at[n, side])
        for side, source in enumerate(sources)
    ]


def square_sums(w_gate, w_up, first, count, halved=False, kept=False):
    _, rows, cols = w_gate.shape
    results = 2 if halved else 1
    height = count // results
    shapes = [jax.ShapeDtypeStruct((2, height, cols), jnp.float32)] * results
    weights = (count, 2, rows, cols)
    if kept:
        shapes.append(jax.ShapeDtypeStruct(weights, jnp.float32))

    def kernel(*refs):
        sources, out_refs = refs[:2], refs[2 : 2 + results]
        held, arrived = refs[2 + results :]
        for n in range(count):
            for copy in fetches(sources, first, held, arrived, n):
                copy.start()
        mine = lax.axis_index("zero") % 2
        for half in range(results):

            @pl.loop(0, height)
            def _(n):
                row = half * height + n
                for side, copy in enumerate(fetches(sources, first, held, arrived, row)):
                    copy.wait()
                    w = held[row, side]
                    found = jnp.sum(w * w, axis=0, keepdims=True)
                    if halved:

                        @pl.when(mine == half)
                        def _():
                            out_refs[0][side, pl.ds(n, 1), :] = found

                        @pl.when(mine != half)
                        def _():
                            out_refs[1][side, pl.ds(n, 1), :] = found

                    else:
                        out_refs[0][side, pl.ds(n, 1), :] = found

    return pl.pallas_call(
        kernel,
        in_specs=[pl.BlockSpec(memory_space=pl.ANY)] * 2,
        out_specs=[pl.BlockSpec(memory_space=pltpu.VMEM)] * len(shapes),
        out_shape=shapes,
        scratch_shapes=([] if kept else [pltpu.VMEM(weights, jnp.float32)]) + [pltpu.SemaphoreType.DMA((count, 2))],
        compiler_params=granted(44),
        cost_estimate=cost(4 * count * rows * cols, 8 * count * rows * cols),
    )(w_gate, w_up)


def scaled_pieces(w_gate, w_up, totals, first, count, start, size):
    _, rows, cols = w_gate.shape
    width = cols // size

    def kernel(gate_ref, up_ref, *refs):
        total_refs, outs, held = refs[: len(totals)], refs[len(totals) : -1], refs[-1]
        me = lax.axis_index("zero")
        step = pl.program_id(0)
        for side, w_ref in enumerate((gate_ref, up_ref)):
            height = totals[0].shape[1]
            half = jnp.where(start + step >= height, 1, 0)
            row = pl.ds(start + step - half * height, 1)
            total = jnp.where(half == me % 2, total_refs[0][side, row, :], total_refs[1][side, row, :])
            inverse = 1.0 / jnp.sqrt(total)
            held[side] = (w_ref[0] * inverse).astype(jnp.bfloat16).T
            for k in range(size):
                offset = pl.multiple_of(lax.bitwise_xor(me, k) * width, width)
                outs[k][side, 0] = held[side, pl.ds(offset, width), :]

    weights = pl.BlockSpec((1, rows, cols), lambda i: (first + i, 0, 0))
    piece = pl.BlockSpec((2, 1, width, rows), lambda i: (0, i, 0, 0))
    return pl.pallas_call(
        kernel,
        grid=(count,),
        in_specs=[weights, weights] + [pl.BlockSpec(memory_space=pltpu.VMEM)] * len(totals),
        out_specs=[piece] * size,
        out_shape=[jax.ShapeDtypeStruct((2, count, width, rows), jnp.bfloat16)] * size,
        scratch_shapes=[pltpu.VMEM((2, cols, rows), jnp.bfloat16)],
        compiler_params=granted(44),
        cost_estimate=cost(4 * count * rows * cols, 12 * count * rows * cols),
    )(w_gate, w_up, *totals)


def scaled_held(weights, totals, start, count, size):
    _, _, rows, cols = weights.shape
    width = cols // size

    def kernel(w_ref, *refs):
        total_refs, outs, held = refs[: len(totals)], refs[len(totals) : -1], refs[-1]
        me = lax.axis_index("zero")
        for n in range(count):
            for side in range(2):
                total = sum(ref[side, pl.ds(start + n, 1), :] for ref in total_refs)
                inverse = 1.0 / jnp.sqrt(total)
                held[n, side] = (w_ref[start + n, side] * inverse).astype(jnp.bfloat16).T
                for k in range(size):
                    offset = pl.multiple_of(lax.bitwise_xor(me, k) * width, width)
                    outs[k][side, n] = held[n, side, pl.ds(offset, width), :]

    return pl.pallas_call(
        kernel,
        in_specs=[pl.BlockSpec(memory_space=pltpu.VMEM)] * (1 + len(totals)),
        out_specs=[pl.BlockSpec(memory_space=pltpu.VMEM)] * size,
        out_shape=[jax.ShapeDtypeStruct((2, count, width, rows), jnp.bfloat16)] * size,
        scratch_shapes=[pltpu.VMEM((count, 2, cols, rows), jnp.bfloat16)],
        compiler_params=granted(44),
        cost_estimate=cost(4 * count * rows * cols, 12 * count * rows * cols),
    )(weights, *totals)


def placed(pieces, outputs, first):
    size = len(pieces)
    _, count, width, rows = pieces[0].shape

    def kernel(*refs):
        ins, outs, left = refs[:size], refs[-3:-1], refs[-1]
        me = lax.axis_index("zero")
        copies = []
        for k in range(size):
            offset = pl.multiple_of(lax.bitwise_xor(me, k) * rows, rows)
            for side in range(2):
                place = outs[side].at[pl.ds(first, count), :, pl.ds(offset, rows)]
                copies.append(pltpu.make_async_copy(ins[k].at[side], place, left.at[k, side]))
        for copy in copies:
            copy.start()
        for copy in copies:
            copy.wait()

    return pl.pallas_call(
        kernel,
        in_specs=[pl.BlockSpec(memory_space=pltpu.VMEM)] * size + [pl.BlockSpec(memory_space=pl.ANY)] * 2,
        out_specs=[pl.BlockSpec(memory_space=pl.ANY)] * 2,
        out_shape=[jax.ShapeDtypeStruct(x.shape, x.dtype) for x in outputs],
        input_output_aliases={size + n: n for n in range(2)},
        scratch_shapes=[pltpu.SemaphoreType.DMA((size, 2))],
        compiler_params=granted(44),
        cost_estimate=cost(count * width * rows * size, 8 * count * width * rows * size),
    )(*pieces, *outputs)


def assembled(pieces, outputs, first, experts):
    size = len(pieces)
    _, count, width, rows = pieces[0].shape

    def kernel(*refs):
        ins, outs = refs[:size], refs[-2:]
        me = lax.axis_index("zero")
        for k in range(size):
            offset = pl.multiple_of(lax.bitwise_xor(me, k) * rows, rows)
            for side in range(2):
                outs[side][0, :, pl.ds(offset, rows)] = ins[k][side, 0]

    piece = pl.BlockSpec((2, 1, width, rows), lambda i: (0, i, 0, 0))
    whole = pl.BlockSpec((1, width, size * rows), lambda i: (first + i, 0, 0))
    kept = () if outputs is None else tuple(outputs)
    return pl.pallas_call(
        kernel,
        grid=(count,),
        in_specs=[piece] * size + [pl.BlockSpec(memory_space=pl.ANY)] * len(kept),
        out_specs=[whole, whole],
        out_shape=[jax.ShapeDtypeStruct((experts, width, size * rows), jnp.bfloat16)] * 2,
        input_output_aliases={size + n: n for n in range(len(kept))},
        compiler_params=granted(44),
        cost_estimate=cost(count * width * rows * size, 8 * count * width * rows * size),
    )(*pieces, *kept)


def joined_rows(pieces):
    size = len(pieces)
    height, rows = pieces[0].shape

    def kernel(*refs):
        me = lax.axis_index("zero")
        for k in range(size):
            offset = pl.multiple_of(lax.bitwise_xor(me, k) * rows, rows)
            refs[size][:, pl.ds(offset, rows)] = refs[k][...]

    return pl.pallas_call(
        kernel,
        out_shape=jax.ShapeDtypeStruct((height, size * rows), pieces[0].dtype),
        cost_estimate=cost(size * height * rows, 4 * size * height * rows),
    )(*pieces)


def joined_columns(pieces):
    banks = len(pieces)
    height, rows = pieces[0].shape

    def kernel(*refs):
        out_ref, held = refs[banks], refs[banks + 1]
        me = lax.axis_index("bank")
        for k in range(banks):
            offset = pl.multiple_of(lax.bitwise_xor(me, k) * height, height)
            held[pl.ds(offset, height), :] = refs[k][...]
        out_ref[...] = held[...].T

    return pl.pallas_call(
        kernel,
        out_shape=jax.ShapeDtypeStruct((rows, banks * height), pieces[0].dtype),
        scratch_shapes=[pltpu.VMEM((banks * height, rows), pieces[0].dtype)],
        cost_estimate=cost(banks * height * rows, 4 * banks * height * rows),
    )(*pieces)


def chunk_sizes(experts):
    unit = experts // 32
    return [[unit * n for n in group] for group in ((2,), (2, 2), (2, 4, 8, 8, 3, 1))]


def piped(w_gate, w_up, router_weight, router_gain, size, banks):
    experts, _, cols = w_gate.shape
    width = cols // size

    def send(x, k, axis="zero", count=size):
        return lax.ppermute(x, axis, xor_pairs(count, k))

    groups = chunk_sizes(experts)
    sizes = [n for group in groups for n in group]
    chunks = range(len(sizes))
    firsts = [sum(sizes[:c]) for c in chunks]

    totals, starts = [], [sum(map(sum, groups[:g])) for g in range(len(groups))]
    last = len(groups) - 1
    kept = []
    for g, group in enumerate(groups[:last]):
        own, weights = square_sums(w_gate, w_up, starts[g], sum(group), kept=True)
        kept.append(weights)
        own = own + send(own, 1)
        totals.append([own] + [send(own, k) for k in range(2, size, 2)])
    own, other = square_sums(w_gate, w_up, starts[last], sum(groups[last]), halved=True)
    own = own + send(other, 1)
    k = 2
    while k < size:
        own = own + send(own, k)
        k *= 2
    totals.append([own, send(own, 1)])

    sent, got = [], []
    for c in chunks:
        group = max(g for g in range(len(groups)) if starts[g] <= firsts[c])
        start = firsts[c] - starts[group]
        if group < last:
            sent.append(scaled_held(kept[group], totals[group], start, sizes[c], size))
        else:
            sent.append(scaled_pieces(w_gate, w_up, totals[group], firsts[c], sizes[c], start, size))
        got.append([sent[c][0]] + [send(sent[c][k], k) for k in range(1, size)])

    part = (router_weight * router_gain[:, None]).astype(jnp.bfloat16).T
    parts = [part, send(part, 1)]
    for k in range(2, size, 2):
        parts.append(send(part, k))
        parts.append(send(parts[k], 1))
    row = joined_rows(parts)
    columns = [row] + [send(row, k, "bank", banks) for k in range(1, banks)]
    serve_router = joined_columns(columns)

    outputs = None
    for c in chunks:
        if c < len(sizes) - 1:
            outputs = assembled(got[c], outputs, firsts[c], experts)
        else:
            outputs = placed(got[c], outputs, firsts[c])
    serve_gate, serve_up = (jnp.swapaxes(x, 1, 2) for x in outputs)

    even = lax.axis_index("zero") % 2 == 0
    low, high = (jnp.where(even, x, y) for x, y in (totals[last], totals[last][::-1]))
    mine = [
        lax.dynamic_slice_in_dim(x, lax.axis_index("zero") * width, width, axis=2)
        for x in [sum(parts) for parts in totals[:last]] + [low, high]
    ]
    scale = jnp.sqrt(jnp.concatenate(mine, axis=1))
    return (serve_gate, serve_up, scale[0], scale[1], serve_router)


def plain(w_gate, w_up, router_weight, router_gain):
    total_gate, total_up = lax.psum(
        (jnp.sum(w_gate * w_gate, axis=1), jnp.sum(w_up * w_up, axis=1)), "zero"
    )
    scale_gate, scale_up = jnp.sqrt(total_gate), jnp.sqrt(total_up)
    served = [
        lax.all_to_all(
            (w / jnp.expand_dims(scale, 1)).astype(jnp.bfloat16), "zero", split_axis=2, concat_axis=1, tiled=True
        )
        for w, scale in ((w_gate, scale_gate), (w_up, scale_up))
    ]
    width = served[0].shape[2]
    start = lax.axis_index("zero") * width
    scales = [lax.dynamic_slice_in_dim(s, start, width, axis=1) for s in (scale_gate, scale_up)]
    part = (router_weight * router_gain[:, None]).astype(jnp.bfloat16)
    row = lax.all_gather(part, "zero", axis=0, tiled=True)
    return (*served, *scales, lax.all_gather(row, "bank", axis=1, tiled=True))


def solution(mesh):
    size, banks = mesh.shape["zero"], mesh.shape["bank"]
    placed = (P("bank", "zero", None), P("bank", "zero", None), P("zero", "bank"), P("zero"))

    def placed_over(shards):
        return jax.shard_map(
            shards,
            mesh=mesh,
            in_specs=placed,
            out_specs=(
                P("bank", None, "zero"),
                P("bank", None, "zero"),
                P("bank", "zero"),
                P("bank", "zero"),
                P(),
            ),
            check_vma=False,
        )

    def whole(w_gate, w_up, router_weight, router_gain):
        experts, rows, cols = w_gate.shape
        powers = size & (size - 1) == 0 and banks & (banks - 1) == 0
        aligned = rows % (128 * size) == 0 and cols % (16 * size) == 0 and router_weight.shape[1] % (16 * banks) == 0
        if not (powers and aligned and size >= 8 and experts % (32 * banks) == 0):
            return placed_over(plain)(w_gate, w_up, router_weight, router_gain)

        def shards(*args):
            return piped(*args, size, banks)

        return placed_over(shards)(w_gate, w_up, router_weight, router_gain)

    return whole
```

```python
import jax
import jax.numpy as jnp
from jax import lax
from jax.experimental import pallas as pl
from jax.experimental.pallas import tpu as pltpu
from jax.sharding import PartitionSpec as P


def xor_pairs(size, k):
    return [(i, i ^ k) for i in range(size)]


def granted(mib):
    return pltpu.CompilerParams(vmem_limit_bytes=mib << 20)


def cost(flops, moved):
    return pl.CostEstimate(flops=flops, bytes_accessed=moved, transcendentals=0)


def fetches(sources, first, held, arrived, n):
    return [
        pltpu.make_async_copy(source.at[first + n], held.at[n, side], arrived.at[n, side])
        for side, source in enumerate(sources)
    ]


def square_sums(w_gate, w_up, first, count, halved=False, kept=False):
    _, rows, cols = w_gate.shape
    results = 2 if halved else 1
    height = count // results
    shapes = [jax.ShapeDtypeStruct((2, height, cols), jnp.float32)] * results
    weights = (count, 2, rows, cols)
    if kept:
        shapes.append(jax.ShapeDtypeStruct(weights, jnp.float32))

    def kernel(*refs):
        sources, out_refs = refs[:2], refs[2 : 2 + results]
        held, arrived = refs[2 + results :]
        for n in range(count):
            for copy in fetches(sources, first, held, arrived, n):
                copy.start()
        mine = lax.axis_index("zero") % 2
        for half in range(results):

            @pl.loop(0, height)
            def _(n):
                row = half * height + n
                for side, copy in enumerate(fetches(sources, first, held, arrived, row)):
                    copy.wait()
                    w = held[row, side]
                    found = jnp.sum(w * w, axis=0, keepdims=True)
                    if halved:

                        @pl.when(mine == half)
                        def _():
                            out_refs[0][side, pl.ds(n, 1), :] = found

                        @pl.when(mine != half)
                        def _():
                            out_refs[1][side, pl.ds(n, 1), :] = found

                    else:
                        out_refs[0][side, pl.ds(n, 1), :] = found

    return pl.pallas_call(
        kernel,
        in_specs=[pl.BlockSpec(memory_space=pl.ANY)] * 2,
        out_specs=[pl.BlockSpec(memory_space=pltpu.VMEM)] * len(shapes),
        out_shape=shapes,
        scratch_shapes=([] if kept else [pltpu.VMEM(weights, jnp.float32)]) + [pltpu.SemaphoreType.DMA((count, 2))],
        compiler_params=granted(44),
        cost_estimate=cost(4 * count * rows * cols, 8 * count * rows * cols),
    )(w_gate, w_up)


def scaled_pieces(w_gate, w_up, totals, first, count, start, size):
    _, rows, cols = w_gate.shape
    width = cols // size

    def kernel(gate_ref, up_ref, *refs):
        total_refs, outs, held = refs[: len(totals)], refs[len(totals) : -1], refs[-1]
        me = lax.axis_index("zero")
        step = pl.program_id(0)
        for side, w_ref in enumerate((gate_ref, up_ref)):
            height = totals[0].shape[1]
            half = jnp.where(start + step >= height, 1, 0)
            row = pl.ds(start + step - half * height, 1)
            total = jnp.where(half == me % 2, total_refs[0][side, row, :], total_refs[1][side, row, :])
            inverse = 1.0 / jnp.sqrt(total)
            held[side] = (w_ref[0] * inverse).astype(jnp.bfloat16).T
            for k in range(size):
                offset = pl.multiple_of(lax.bitwise_xor(me, k) * width, width)
                outs[k][side, 0] = held[side, pl.ds(offset, width), :]

    weights = pl.BlockSpec((1, rows, cols), lambda i: (first + i, 0, 0))
    piece = pl.BlockSpec((2, 1, width, rows), lambda i: (0, i, 0, 0))
    return pl.pallas_call(
        kernel,
        grid=(count,),
        in_specs=[weights, weights] + [pl.BlockSpec(memory_space=pltpu.VMEM)] * len(totals),
        out_specs=[piece] * size,
        out_shape=[jax.ShapeDtypeStruct((2, count, width, rows), jnp.bfloat16)] * size,
        scratch_shapes=[pltpu.VMEM((2, cols, rows), jnp.bfloat16)],
        compiler_params=granted(44),
        cost_estimate=cost(4 * count * rows * cols, 12 * count * rows * cols),
    )(w_gate, w_up, *totals)


def scaled_held(weights, totals, start, count, size):
    _, _, rows, cols = weights.shape
    width = cols // size

    def kernel(w_ref, *refs):
        total_refs, outs, held = refs[: len(totals)], refs[len(totals) : -1], refs[-1]
        me = lax.axis_index("zero")
        for n in range(count):
            for side in range(2):
                total = sum(ref[side, pl.ds(start + n, 1), :] for ref in total_refs)
                inverse = 1.0 / jnp.sqrt(total)
                held[n, side] = (w_ref[start + n, side] * inverse).astype(jnp.bfloat16).T
                for k in range(size):
                    offset = pl.multiple_of(lax.bitwise_xor(me, k) * width, width)
                    outs[k][side, n] = held[n, side, pl.ds(offset, width), :]

    return pl.pallas_call(
        kernel,
        in_specs=[pl.BlockSpec(memory_space=pltpu.VMEM)] * (1 + len(totals)),
        out_specs=[pl.BlockSpec(memory_space=pltpu.VMEM)] * size,
        out_shape=[jax.ShapeDtypeStruct((2, count, width, rows), jnp.bfloat16)] * size,
        scratch_shapes=[pltpu.VMEM((count, 2, cols, rows), jnp.bfloat16)],
        compiler_params=granted(44),
        cost_estimate=cost(4 * count * rows * cols, 12 * count * rows * cols),
    )(weights, *totals)


def placed(pieces, outputs, first):
    size = len(pieces)
    _, count, width, rows = pieces[0].shape

    def kernel(*refs):
        ins, outs, (held, arrived, left) = refs[:size], refs[-5:-3], refs[-3:]
        me = lax.axis_index("zero")
        places = [(side, k) for side in range(2) for k in range(size)]

        def arrival(side, k):
            return pltpu.make_async_copy(ins[k].at[side], held.at[k, side], arrived.at[k, side])

        def departure(side, k):
            offset = pl.multiple_of(lax.bitwise_xor(me, k) * rows, rows)
            place = outs[side].at[pl.ds(first, count), :, pl.ds(offset, rows)]
            return pltpu.make_async_copy(held.at[k, side], place, left.at[k, side])

        for place in places:
            arrival(*place).start()
        for place in places:
            arrival(*place).wait()
            departure(*place).start()
        for place in places:
            departure(*place).wait()

    return pl.pallas_call(
        kernel,
        in_specs=[pl.BlockSpec(memory_space=pl.ANY)] * (size + 2),
        out_specs=[pl.BlockSpec(memory_space=pl.ANY)] * 2,
        out_shape=[jax.ShapeDtypeStruct(x.shape, x.dtype) for x in outputs],
        input_output_aliases={size + n: n for n in range(2)},
        scratch_shapes=[
            pltpu.VMEM((size, 2, count, width, rows), jnp.bfloat16),
            pltpu.SemaphoreType.DMA((size, 2)),
            pltpu.SemaphoreType.DMA((size, 2)),
        ],
        compiler_params=granted(44),
        cost_estimate=cost(count * width * rows * size, 8 * count * width * rows * size),
    )(*pieces, *outputs)


def assembled(pieces, outputs, first, experts):
    size = len(pieces)
    _, count, width, rows = pieces[0].shape

    def kernel(*refs):
        ins, outs = refs[:size], refs[-2:]
        me = lax.axis_index("zero")
        for k in range(size):
            offset = pl.multiple_of(lax.bitwise_xor(me, k) * rows, rows)
            for side in range(2):
                outs[side][0, :, pl.ds(offset, rows)] = ins[k][side, 0]

    piece = pl.BlockSpec((2, 1, width, rows), lambda i: (0, i, 0, 0))
    whole = pl.BlockSpec((1, width, size * rows), lambda i: (first + i, 0, 0))
    kept = () if outputs is None else tuple(outputs)
    return pl.pallas_call(
        kernel,
        grid=(count,),
        in_specs=[piece] * size + [pl.BlockSpec(memory_space=pl.ANY)] * len(kept),
        out_specs=[whole, whole],
        out_shape=[jax.ShapeDtypeStruct((experts, width, size * rows), jnp.bfloat16)] * 2,
        input_output_aliases={size + n: n for n in range(len(kept))},
        compiler_params=granted(44),
        cost_estimate=cost(count * width * rows * size, 8 * count * width * rows * size),
    )(*pieces, *kept)


def joined_rows(pieces):
    size = len(pieces)
    height, rows = pieces[0].shape

    def kernel(*refs):
        me = lax.axis_index("zero")
        for k in range(size):
            offset = pl.multiple_of(lax.bitwise_xor(me, k) * rows, rows)
            refs[size][:, pl.ds(offset, rows)] = refs[k][...]

    return pl.pallas_call(
        kernel,
        out_shape=jax.ShapeDtypeStruct((height, size * rows), pieces[0].dtype),
        cost_estimate=cost(size * height * rows, 4 * size * height * rows),
    )(*pieces)


def joined_columns(pieces):
    banks = len(pieces)
    height, rows = pieces[0].shape

    def kernel(*refs):
        out_ref, held = refs[banks], refs[banks + 1]
        me = lax.axis_index("bank")
        for k in range(banks):
            offset = pl.multiple_of(lax.bitwise_xor(me, k) * height, height)
            held[pl.ds(offset, height), :] = refs[k][...]
        out_ref[...] = held[...].T

    return pl.pallas_call(
        kernel,
        out_shape=jax.ShapeDtypeStruct((rows, banks * height), pieces[0].dtype),
        scratch_shapes=[pltpu.VMEM((banks * height, rows), pieces[0].dtype)],
        cost_estimate=cost(banks * height * rows, 4 * banks * height * rows),
    )(*pieces)


def chunk_sizes(experts):
    unit = experts // 32
    return [[unit * n for n in group] for group in ((2,), (2, 2), (2, 4, 8, 8, 3, 1))]


def piped(w_gate, w_up, router_weight, router_gain, size, banks):
    experts, _, cols = w_gate.shape
    width = cols // size

    def send(x, k, axis="zero", count=size):
        return lax.ppermute(x, axis, xor_pairs(count, k))

    groups = chunk_sizes(experts)
    sizes = [n for group in groups for n in group]
    chunks = range(len(sizes))
    firsts = [sum(sizes[:c]) for c in chunks]

    totals, starts = [], [sum(map(sum, groups[:g])) for g in range(len(groups))]
    last = len(groups) - 1
    kept = []
    for g, group in enumerate(groups[:last]):
        own, weights = square_sums(w_gate, w_up, starts[g], sum(group), kept=True)
        kept.append(weights)
        own = own + send(own, 1)
        totals.append([own] + [send(own, k) for k in range(2, size, 2)])
    own, other = square_sums(w_gate, w_up, starts[last], sum(groups[last]), halved=True)
    own = own + send(other, 1)
    k = 2
    while k < size:
        own = own + send(own, k)
        k *= 2
    totals.append([own, send(own, 1)])

    sent, got = [], []
    for c in chunks:
        group = max(g for g in range(len(groups)) if starts[g] <= firsts[c])
        start = firsts[c] - starts[group]
        if group < last:
            sent.append(scaled_held(kept[group], totals[group], start, sizes[c], size))
        else:
            sent.append(scaled_pieces(w_gate, w_up, totals[group], firsts[c], sizes[c], start, size))
        got.append([sent[c][0]] + [send(sent[c][k], k) for k in range(1, size)])

    part = (router_weight * router_gain[:, None]).astype(jnp.bfloat16).T
    parts = [part, send(part, 1)]
    for k in range(2, size, 2):
        parts.append(send(part, k))
        parts.append(send(parts[k], 1))
    row = joined_rows(parts)
    columns = [row] + [send(row, k, "bank", banks) for k in range(1, banks)]
    serve_router = joined_columns(columns)

    outputs = None
    for c in chunks:
        if c < len(sizes) - 1:
            outputs = assembled(got[c], outputs, firsts[c], experts)
        else:
            outputs = placed(got[c], outputs, firsts[c])
    serve_gate, serve_up = (jnp.swapaxes(x, 1, 2) for x in outputs)

    even = lax.axis_index("zero") % 2 == 0
    low, high = (jnp.where(even, x, y) for x, y in (totals[last], totals[last][::-1]))
    mine = [
        lax.dynamic_slice_in_dim(x, lax.axis_index("zero") * width, width, axis=2)
        for x in [sum(parts) for parts in totals[:last]] + [low, high]
    ]
    scale = jnp.sqrt(jnp.concatenate(mine, axis=1))
    return (serve_gate, serve_up, scale[0], scale[1], serve_router)


def plain(w_gate, w_up, router_weight, router_gain):
    total_gate, total_up = lax.psum(
        (jnp.sum(w_gate * w_gate, axis=1), jnp.sum(w_up * w_up, axis=1)), "zero"
    )
    scale_gate, scale_up = jnp.sqrt(total_gate), jnp.sqrt(total_up)
    served = [
        lax.all_to_all(
            (w / jnp.expand_dims(scale, 1)).astype(jnp.bfloat16), "zero", split_axis=2, concat_axis=1, tiled=True
        )
        for w, scale in ((w_gate, scale_gate), (w_up, scale_up))
    ]
    width = served[0].shape[2]
    start = lax.axis_index("zero") * width
    scales = [lax.dynamic_slice_in_dim(s, start, width, axis=1) for s in (scale_gate, scale_up)]
    part = (router_weight * router_gain[:, None]).astype(jnp.bfloat16)
    row = lax.all_gather(part, "zero", axis=0, tiled=True)
    return (*served, *scales, lax.all_gather(row, "bank", axis=1, tiled=True))


def solution(mesh):
    size, banks = mesh.shape["zero"], mesh.shape["bank"]
    placed = (P("bank", "zero", None), P("bank", "zero", None), P("zero", "bank"), P("zero"))

    def placed_over(shards):
        return jax.shard_map(
            shards,
            mesh=mesh,
            in_specs=placed,
            out_specs=(
                P("bank", None, "zero"),
                P("bank", None, "zero"),
                P("bank", "zero"),
                P("bank", "zero"),
                P(),
            ),
            check_vma=False,
        )

    def whole(w_gate, w_up, router_weight, router_gain):
        experts, rows, cols = w_gate.shape
        powers = size & (size - 1) == 0 and banks & (banks - 1) == 0
        aligned = rows % (128 * size) == 0 and cols % (16 * size) == 0 and router_weight.shape[1] % (16 * banks) == 0
        if not (powers and aligned and size >= 8 and experts % (32 * banks) == 0):
            return placed_over(plain)(w_gate, w_up, router_weight, router_gain)

        def shards(*args):
            return piped(*args, size, banks)

        return placed_over(shards)(w_gate, w_up, router_weight, router_gain)

    return whole
```
